8 devices in a mesh: dp: 2 (over z, y), vp: 4 (over x, core).
Axes of the slice: x: 2, y: 2, z: 1, core: 2. Of those that a mesh axis runs over, the one named last changes fastest.
Arguments:
- hidden: bfloat16 [6, 256, 896], P('dp')
- norm_gain: float32 [896], replicated
- emb_table: bfloat16 [151936, 896], P('vp')
- labels: int32 [6, 256], P('dp')
- tok_mask: float32 [6, 256], P('dp')
Outputs:
- output 1: float32 [], replicated
- output 2: float32 [151936, 896], P('vp')
- output 3: bfloat16 [6, 256, 896], P('dp')
- output 4: float32 [896], replicated
All inputs are finite; a program needn't handle non-finite values.
Results may differ from the reference program's by a relative error of at most 0.001.
Values sent between devices are 32-bit elements.
A program may use at most 1 GiB of HBM per device.

```python
import math
import jax
import jax.numpy as jnp
from jax import lax

WIDTH = 896
VOCAB = 151936
BATCH = 6
SEQ_LEN = 256
LOGIT_SCALE = 0.0625
EPS = 1e-5
EMB_GAIN = 48.0
TARGET_PULL = 4.0
BLOCK_ROWS = math.gcd(BATCH, max(1, 2**25 // (SEQ_LEN * VOCAB)))
NUM_BLOCKS = BATCH // BLOCK_ROWS
BLOCK_TOKENS = BLOCK_ROWS * SEQ_LEN


def setup_inputs(seed: int = 0) -> dict:
    key = jax.random.key(seed)
    key_table, key_noise, key_gain, key_labels, key_lengths = jax.random.split(key, 5)
    emb_std = EMB_GAIN / math.sqrt(WIDTH)
    emb_table = (jax.random.normal(key_table, (VOCAB, WIDTH), jnp.float32) * emb_std).astype(jnp.bfloat16)
    labels = jax.random.randint(key_labels, (BATCH, SEQ_LEN), 0, VOCAB, dtype=jnp.int32)
    target_rows = jnp.take(emb_table, labels, axis=0).astype(jnp.float32) / emb_std
    noise = jax.random.normal(key_noise, (BATCH, SEQ_LEN, WIDTH), jnp.float32)
    hidden = (noise + (TARGET_PULL / math.sqrt(WIDTH)) * target_rows).astype(jnp.bfloat16)
    lengths = jax.random.randint(key_lengths, (BATCH, 1), max(1, SEQ_LEN // 4), SEQ_LEN + 1, dtype=jnp.int32)
    tok_mask = (jnp.arange(SEQ_LEN)[None, :] < lengths).astype(jnp.float32)
    norm_gain = 1.0 + 0.25 * jax.random.normal(key_gain, (WIDTH,), jnp.float32)
    return {'hidden': hidden, 'norm_gain': norm_gain, 'emb_table': emb_table, 'labels': labels, 'tok_mask': tok_mask}


def norm_forward(tokens, norm_gain):
    values = tokens.astype(jnp.float32)
    mean_x = jnp.mean(values, axis=-1, keepdims=True)
    centered = values - mean_x
    variance = jnp.mean(centered * centered, axis=-1, keepdims=True)
    inv_std = lax.rsqrt(variance + EPS)
    x_hat = centered * inv_std
    return (norm_gain * x_hat).astype(jnp.bfloat16), x_hat, inv_std


def reference(hidden, norm_gain, emb_table, labels, tok_mask):
    count = jnp.sum(tok_mask)
    vocab_ids = jnp.arange(VOCAB)

    def block_step(carry, block):
        table_grad, gain_grad, loss_sum = carry
        tokens, block_labels, block_mask = block
        normed, x_hat, inv_std = norm_forward(tokens, norm_gain)
        logits = LOGIT_SCALE * jnp.dot(normed, emb_table.T, preferred_element_type=jnp.float32)
        log_norm = jax.nn.logsumexp(logits, axis=-1)
        hits = vocab_ids[None, :] == block_labels[:, None]
        label_logit = jnp.sum(jnp.where(hits, logits, 0.0), axis=-1)
        loss_sum = loss_sum + jnp.sum(block_mask * (log_norm - label_logit))
        soft_probs = jnp.exp(logits - log_norm[:, None])
        weight = block_mask * (LOGIT_SCALE / count)
        d_logits = (jnp.where(hits, soft_probs - 1.0, soft_probs) * weight[:, None]).astype(jnp.bfloat16)
        d_normed = jnp.dot(d_logits, emb_table, preferred_element_type=jnp.float32)
        table_grad = table_grad + jnp.dot(d_logits.T, normed, preferred_element_type=jnp.float32)
        gain_grad = gain_grad + jnp.sum(d_normed * x_hat, axis=0)
        d_xhat = d_normed * norm_gain
        mean_one = jnp.mean(d_xhat, axis=-1, keepdims=True)
        mean_two = jnp.mean(d_xhat * x_hat, axis=-1, keepdims=True)
        d_tokens = inv_std * (d_xhat - mean_one - x_hat * mean_two)
        return (table_grad, gain_grad, loss_sum), d_tokens.astype(jnp.bfloat16)

    blocks = (hidden.reshape(NUM_BLOCKS, BLOCK_TOKENS, WIDTH), labels.reshape(NUM_BLOCKS, BLOCK_TOKENS), tok_mask.reshape(NUM_BLOCKS, BLOCK_TOKENS))
    start = (jnp.zeros((VOCAB, WIDTH), jnp.float32), jnp.zeros((WIDTH,), jnp.float32), jnp.zeros((), jnp.float32))
    (table_grad, gain_grad, loss_sum), d_tokens = lax.scan(block_step, start, blocks)
    return loss_sum / count, table_grad, d_tokens.reshape(BATCH, SEQ_LEN, WIDTH), gain_grad
```

```python
import functools

import jax
import jax.numpy as jnp
from jax import lax
from jax.experimental import pallas as pl
from jax.experimental.pallas import tpu as pltpu
from jax.sharding import PartitionSpec as P

LOGIT_SCALE = 0.0625
EPS = 1e-5
LOG2E = 1.4426950408889634
LN2 = 0.6931471805599453
NEG = -1e30
TILE = 256
VMEM = 63 * 2**20


def logits_kernel(vocab, bv, rc, e_ref, nt_ref, z_ref, m_ref, s_ref):
    i = pl.program_id(0)

    @pl.when(i == 0)
    def _():
        m_ref[...] = jnp.full(m_ref.shape, NEG, jnp.float32)
        s_ref[...] = jnp.zeros(s_ref.shape, jnp.float32)

    width = nt_ref.shape[1]
    limit = vocab - i * bv
    for r in range(0, bv, rc):
        z = jnp.dot(e_ref[pl.ds(r, rc), :], nt_ref[...], preferred_element_type=jnp.float32)
        rows = lax.broadcasted_iota(jnp.int32, (rc, width), 0) + r
        z = jnp.where(rows < limit, z * (LOGIT_SCALE * LOG2E), NEG)
        z_ref[pl.ds(r, rc), :] = z
        groups = z.reshape(rc // 8, 8, width)
        old = m_ref[...]
        new = jnp.maximum(old, jnp.max(groups, axis=0))
        s_ref[...] = s_ref[...] * jnp.exp2(old - new) + jnp.sum(jnp.exp2(groups - new[None]), axis=0)
        m_ref[...] = new


def logits_call(nt, bv, rc, table, normed_t):
    vocab, depth = table.shape
    steps = pl.cdiv(vocab, bv)
    width = nt * TILE
    full = normed_t.shape[1]
    fixed = lambda i: (0, 0)
    return pl.pallas_call(
        functools.partial(logits_kernel, vocab, bv, rc),
        grid=(steps,),
        in_specs=[pl.BlockSpec((bv, depth), lambda i: (i, 0)), pl.BlockSpec((depth, width), fixed)],
        out_specs=[pl.BlockSpec((bv, width), lambda i: (i, 0)), pl.BlockSpec((8, width), fixed), pl.BlockSpec((8, width), fixed)],
        out_shape=[
            jax.ShapeDtypeStruct((steps * bv, full), jnp.float32),
            jax.ShapeDtypeStruct((8, full), jnp.float32),
            jax.ShapeDtypeStruct((8, full), jnp.float32),
        ],
        compiler_params=pltpu.CompilerParams(dimension_semantics=("arbitrary",), vmem_limit_bytes=VMEM),
        name=f"logits_{nt}",
    )(table, normed_t)


def grad_kernel(vocab, bv, rc, nt, own, info_ref, z_ref, e_ref, n_ref, lw_ref, w_ref, lab_ref, dt_ref, dn_ref, lz_ref, dz_ref, et_ref):
    i = pl.program_id(0)

    @pl.when(i == 0)
    def _():
        dn_ref[...] = jnp.zeros(dn_ref.shape, jnp.float32)
        lz_ref[...] = jnp.zeros(lz_ref.shape, jnp.float32)

    width = nt * TILE
    limit = vocab - i * bv
    labels = lab_ref[...] - i * bv
    lw = lw_ref[...]
    w = w_ref[...]
    for r in range(0, bv, rc):
        z = z_ref[pl.ds(r, rc), :]
        hit = lax.broadcasted_iota(jnp.int32, (rc, width), 0) + r == labels
        dz = (jnp.exp2(z - lw) - jnp.where(hit, w, 0.0)).astype(jnp.bfloat16)
        lz_ref[...] += jnp.sum(jnp.where(hit, z, 0.0).reshape(rc // 8, 8, width), axis=0)
        dz_ref[pl.ds(r, rc), :] = dz
        dt_ref[pl.ds(r, rc), :] = jnp.dot(dz, n_ref[...], preferred_element_type=jnp.float32)
    rows = lax.broadcasted_iota(jnp.int32, e_ref.shape, 0)
    et_ref[...] = jnp.where(rows < limit, e_ref[...], jnp.zeros((), jnp.bfloat16)).T
    for j in range(own):
        @pl.when(j < info_ref[0])
        def _():
            at = jnp.where(info_ref[1] == 0, j, nt - 1 - j)
            cols = pl.ds(pl.multiple_of(at * TILE, TILE), TILE)
            dn_ref[:, j * TILE:(j + 1) * TILE] += jnp.dot(et_ref[...], dz_ref[:, cols], preferred_element_type=jnp.float32)


def grad_call(nt, bv, rc, own_max, info, z, table, normed, lw, w, labels):
    vocab, depth = table.shape
    steps = pl.cdiv(vocab, bv)
    width = nt * TILE
    full = normed.shape[0]
    own = min(nt, own_max)
    fixed = lambda i, *_: (0, 0)
    step = lambda i, *_: (i, 0)
    return pl.pallas_call(
        functools.partial(grad_kernel, vocab, bv, rc, nt, own),
        grid_spec=pltpu.PrefetchScalarGridSpec(
            num_scalar_prefetch=1,
            grid=(steps,),
            in_specs=[
                pl.BlockSpec((bv, width), step),
                pl.BlockSpec((bv, depth), step),
                pl.BlockSpec((width, depth), fixed),
                pl.BlockSpec((1, width), fixed),
                pl.BlockSpec((1, width), fixed),
                pl.BlockSpec((1, width), fixed),
            ],
            out_specs=[pl.BlockSpec((bv, depth), step), pl.BlockSpec((depth, own_max * TILE), fixed), pl.BlockSpec((8, width), fixed)],
            scratch_shapes=[pltpu.VMEM((bv, width), jnp.bfloat16), pltpu.VMEM((depth, bv), jnp.bfloat16)],
        ),
        out_shape=[
            jax.ShapeDtypeStruct((vocab, depth), jnp.float32),
            jax.ShapeDtypeStruct((depth, own_max * TILE), jnp.float32),
            jax.ShapeDtypeStruct((8, full), jnp.float32),
        ],
        compiler_params=pltpu.CompilerParams(dimension_semantics=("arbitrary",), vmem_limit_bytes=VMEM),
        name=f"grads_{nt}",
    )(info, z, table, normed, lw, w, labels)


def norm_bwd_kernel(dn_ref, h_ref, gain_ref, slot_ref, dh_ref, dg_ref):
    tokens, depth = h_ref.shape
    slots = dn_ref.shape[1]
    pick = (lax.broadcasted_iota(jnp.int32, (tokens, slots), 1) == slot_ref[...]).astype(jnp.bfloat16)
    h = lax.dot_general(h_ref[...], pick, (((0,), (0,)), ((), ())), preferred_element_type=jnp.float32)
    mu = jnp.mean(h, axis=0, keepdims=True)
    centered = h - mu
    var = jnp.mean(centered * centered, axis=0, keepdims=True)
    inv = lax.rsqrt(var + EPS)
    xhat = centered * inv
    dn = dn_ref[...]
    dg_ref[...] = jnp.sum(dn * xhat, axis=1, keepdims=True)
    a = dn * gain_ref[...]
    one = jnp.mean(a, axis=0, keepdims=True)
    two = jnp.mean(a * xhat, axis=0, keepdims=True)
    dh = (inv * (a - one - xhat * two)).astype(jnp.bfloat16)
    dh_ref[...] = lax.dot_general(pick, dh, (((1,), (1,)), ((), ())), preferred_element_type=jnp.float32).astype(jnp.bfloat16)


def norm_bwd_call(dn, h, gain, slot):
    tokens, depth = h.shape
    return pl.pallas_call(
        norm_bwd_kernel,
        out_shape=[jax.ShapeDtypeStruct((tokens, depth), jnp.bfloat16), jax.ShapeDtypeStruct((depth, 1), jnp.float32)],
        compiler_params=pltpu.CompilerParams(vmem_limit_bytes=VMEM),
        name="norm_bwd",
    )(dn, h, gain.reshape(depth, 1), slot.reshape(tokens, 1))


def solution(mesh):
    def local_step(hidden, norm_gain, emb_table, labels, tok_mask):
        rows, seq_len, depth = hidden.shape
        vocab_local = emb_table.shape[0]
        own = rows * seq_len
        dp = lax.axis_index("dp")
        vp = lax.axis_index("vp")
        flat = hidden.reshape(own, depth)
        values = lax.all_gather(flat.astype(jnp.float32), "dp", axis=0, tiled=True)
        all_labels = lax.all_gather(labels.reshape(own), "dp", axis=0, tiled=True)
        all_mask = lax.all_gather(tok_mask.reshape(own), "dp", axis=0, tiled=True)
        total = all_labels.shape[0]
        max_tiles = total // TILE

        count = jnp.sum(all_mask)
        ranks = jnp.cumsum(all_mask.astype(jnp.int32))
        n_total = ranks[-1]
        n_first = ranks[own - 1]
        tiles = jnp.maximum((n_total + TILE - 1) // TILE, max_tiles // 2)
        token = jnp.arange(total)
        place = jnp.where(token < own, ranks - 1, tiles * TILE - n_total + ranks - 1)
        place = jnp.where(all_mask > 0, place, -1)

        mu = jnp.mean(values, axis=-1, keepdims=True)
        centered = values - mu
        var = jnp.mean(centered * centered, axis=-1, keepdims=True)
        normed = (norm_gain * (centered * lax.rsqrt(var + EPS))).astype(jnp.bfloat16)
        chosen = place[None, :] == jnp.arange(total)[:, None]
        pick = chosen.astype(jnp.bfloat16)
        packed = jnp.dot(pick, normed, preferred_element_type=jnp.float32).astype(jnp.bfloat16)
        packed_t = lax.dot_general(normed, pick, (((0,), (1,)), ((), ())), preferred_element_type=jnp.float32).astype(jnp.bfloat16)
        packed_labels = jnp.sum(jnp.where(chosen, all_labels[None, :], 0), axis=1)
        live = jnp.sum(jnp.where(chosen, 1, 0), axis=1) > 0

        which = jnp.clip(tiles - max_tiles // 2, 0, max_tiles - max_tiles // 2)
        variants = range(max_tiles // 2, max_tiles + 1)
        z, m8, s8 = lax.switch(which, [functools.partial(logits_call, nt, 1536 if nt < 6 else 1280, 128) for nt in variants], emb_table, packed_t)
        m1 = jnp.max(m8, axis=0)
        s1 = jnp.sum(s8 * jnp.exp2(m8 - m1[None]), axis=0)
        ms = lax.all_gather(jnp.stack([m1, s1]), "vp", axis=0)
        m = jnp.max(ms[:, 0], axis=0)
        s = jnp.sum(ms[:, 1] * jnp.exp2(ms[:, 0] - m[None]), axis=0)
        lse = m + jnp.log2(s)
        weight = LOGIT_SCALE / count
        lw = jnp.where(live, lse - jnp.log2(weight), -NEG)
        w = jnp.where(live, weight, 0.0)
        rel_labels = packed_labels - vp * vocab_local
        rel_labels = jnp.where(live & (rel_labels < vocab_local), rel_labels, -1)

        n_own = jnp.where(dp == 0, n_first, n_total - n_first)
        info = jnp.stack([(n_own + TILE - 1) // TILE, dp]).astype(jnp.int32)
        row = lambda x: x.reshape(1, total)
        d_table, dn_t, lz = lax.switch(
            which,
            [functools.partial(grad_call, nt, 1536 if nt < 6 else 1280, 256, own // TILE) for nt in variants],
            info, z, emb_table, packed, row(lw), row(w), row(rel_labels),
        )
        dn_t = lax.psum(dn_t, "vp")
        own_place = lax.dynamic_slice(place, (dp * own,), (own,))
        mirrored = (tiles - 1 - own_place // TILE) * TILE + own_place % TILE
        slot = jnp.where(own_place < 0, -1, jnp.where(dp == 0, own_place, mirrored))
        d_tokens, d_gain = norm_bwd_call(dn_t, flat, norm_gain, slot)

        label_sum = jnp.sum(jnp.where(live, jnp.sum(lz, axis=0), 0.0))
        small = jnp.concatenate([jnp.where(vp == 0, d_gain.reshape(depth), 0.0), jnp.where(dp == 0, label_sum, 0.0).reshape(1)])
        small = lax.psum(small, ("dp", "vp"))
        loss = (jnp.sum(jnp.where(live, lse, 0.0)) - small[depth]) * LN2 / count
        return loss, d_table, d_tokens.reshape(rows, seq_len, depth), small[:depth]

    return jax.shard_map(
        local_step,
        mesh=mesh,
        in_specs=(P("dp", None, None), P(None), P("vp", None), P("dp", None), P("dp", None)),
        out_specs=(P(), P("vp", None), P("dp", None, None), P(None)),
        check_vma=False,
    )
```

```python
import functools

import jax
import jax.numpy as jnp
from jax import lax
from jax.experimental import pallas as pl
from jax.experimental.pallas import tpu as pltpu
from jax.sharding import PartitionSpec as P

LOGIT_SCALE = 0.0625
EPS = 1e-5
LOG2E = 1.4426950408889634
LN2 = 0.6931471805599453
NEG = -1e30
TILE = 256
VMEM = 63 * 2**20


def logits_kernel(vocab, bv, rc, e_ref, nt_ref, z_ref, ms_ref, m_ref, s_ref):
    i = pl.program_id(0)

    @pl.when(i == 0)
    def _():
        m_ref[...] = jnp.full(m_ref.shape, NEG, jnp.float32)
        s_ref[...] = jnp.zeros(s_ref.shape, jnp.float32)

    width = nt_ref.shape[1]
    limit = vocab - i * bv
    for r in range(0, bv, rc):
        z = jnp.dot(e_ref[pl.ds(r, rc), :], nt_ref[...], preferred_element_type=jnp.float32)
        rows = lax.broadcasted_iota(jnp.int32, (rc, width), 0) + r
        z = jnp.where(rows < limit, z * (LOGIT_SCALE * LOG2E), NEG)
        z_ref[pl.ds(r, rc), :] = z
        groups = z.reshape(rc // 8, 8, width)
        old = m_ref[...]
        new = jnp.maximum(old, jnp.max(groups, axis=0))
        s_ref[...] = s_ref[...] * jnp.exp2(old - new) + jnp.sum(jnp.exp2(groups - new[None]), axis=0)
        m_ref[...] = new

    @pl.when(i == pl.num_programs(0) - 1)
    def _():
        best = jnp.max(m_ref[...], axis=0, keepdims=True)
        ms_ref[0:1, :] = best
        ms_ref[1:2, :] = jnp.sum(s_ref[...] * jnp.exp2(m_ref[...] - best), axis=0, keepdims=True)


def logits_call(nt, bv, rc, table, normed_t):
    vocab, depth = table.shape
    steps = pl.cdiv(vocab, bv)
    width = nt * TILE
    full = normed_t.shape[1]
    fixed = lambda i: (0, 0)
    return pl.pallas_call(
        functools.partial(logits_kernel, vocab, bv, rc),
        grid=(steps,),
        in_specs=[pl.BlockSpec((bv, depth), lambda i: (i, 0)), pl.BlockSpec((depth, width), fixed)],
        out_specs=[pl.BlockSpec((bv, width), lambda i: (i, 0)), pl.BlockSpec((8, width), fixed)],
        out_shape=[jax.ShapeDtypeStruct((steps * bv, full), jnp.float32), jax.ShapeDtypeStruct((8, full), jnp.float32)],
        scratch_shapes=[pltpu.VMEM((8, width), jnp.float32), pltpu.VMEM((8, width), jnp.float32)],
        compiler_params=pltpu.CompilerParams(dimension_semantics=("arbitrary",), vmem_limit_bytes=VMEM),
        name=f"logits_{nt}",
    )(table, normed_t)


def grad_kernel(vocab, bv, rc, nt, own, info_ref, z_ref, e_ref, n_ref, lw_ref, w_ref, lab_ref, dt_ref, dn_ref, lz_ref, dz_ref, et_ref):
    i = pl.program_id(0)

    @pl.when(i == 0)
    def _():
        dn_ref[...] = jnp.zeros(dn_ref.shape, jnp.float32)
        lz_ref[...] = jnp.zeros(lz_ref.shape, jnp.float32)

    width = nt * TILE
    limit = vocab - i * bv
    labels = lab_ref[...] - i * bv
    lw = lw_ref[...]
    w = w_ref[...]
    for r in range(0, bv, rc):
        z = z_ref[pl.ds(r, rc), :]
        hit = lax.broadcasted_iota(jnp.int32, (rc, width), 0) + r == labels
        dz = (jnp.exp2(z - lw) - jnp.where(hit, w, 0.0)).astype(jnp.bfloat16)
        lz_ref[...] += jnp.sum(jnp.where(hit, z, 0.0).reshape(rc // 8, 8, width), axis=0)
        dz_ref[pl.ds(r, rc), :] = dz
        dt_ref[pl.ds(r, rc), :] = jnp.dot(dz, n_ref[...], preferred_element_type=jnp.float32)
    rows = lax.broadcasted_iota(jnp.int32, e_ref.shape, 0)
    et_ref[...] = jnp.where(rows < limit, e_ref[...], jnp.zeros((), jnp.bfloat16)).T
    for j in range(own):
        @pl.when(j < info_ref[0])
        def _():
            at = jnp.where(info_ref[1] == 0, j, nt - 1 - j)
            cols = pl.ds(pl.multiple_of(at * TILE, TILE), TILE)
            dn_ref[:, j * TILE:(j + 1) * TILE] += jnp.dot(et_ref[...], dz_ref[:, cols], preferred_element_type=jnp.float32)


def grad_call(nt, bv, rc, own_max, info, z, table, normed, lw, w, labels):
    vocab, depth = table.shape
    steps = pl.cdiv(vocab, bv)
    width = nt * TILE
    full = normed.shape[0]
    own = min(nt, own_max)
    fixed = lambda i, *_: (0, 0)
    step = lambda i, *_: (i, 0)
    return pl.pallas_call(
        functools.partial(grad_kernel, vocab, bv, rc, nt, own),
        grid_spec=pltpu.PrefetchScalarGridSpec(
            num_scalar_prefetch=1,
            grid=(steps,),
            in_specs=[
                pl.BlockSpec((bv, width), step),
                pl.BlockSpec((bv, depth), step),
                pl.BlockSpec((width, depth), fixed),
                pl.BlockSpec((1, width), fixed),
                pl.BlockSpec((1, width), fixed),
                pl.BlockSpec((1, width), fixed),
            ],
            out_specs=[pl.BlockSpec((bv, depth), step), pl.BlockSpec((depth, own_max * TILE), fixed), pl.BlockSpec((8, width), fixed)],
            scratch_shapes=[pltpu.VMEM((bv, width), jnp.bfloat16), pltpu.VMEM((depth, bv), jnp.bfloat16)],
        ),
        out_shape=[
            jax.ShapeDtypeStruct((vocab, depth), jnp.float32),
            jax.ShapeDtypeStruct((depth, own_max * TILE), jnp.float32),
            jax.ShapeDtypeStruct((8, full), jnp.float32),
        ],
        compiler_params=pltpu.CompilerParams(dimension_semantics=("arbitrary",), vmem_limit_bytes=VMEM),
        name=f"grads_{nt}",
    )(info, z, table, normed, lw, w, labels)


MESH = pl.DeviceIdType.MESH


def greet(peers):
    barrier = pltpu.get_barrier_semaphore()
    for peer in peers:
        pl.semaphore_signal(barrier, inc=1, device_id=peer, device_id_type=MESH)
    pl.semaphore_wait(barrier, len(peers))


def remote(src, dst, sems, peer):
    return pltpu.make_async_remote_copy(
        src_ref=src, dst_ref=dst, send_sem=sems[0], recv_sem=sems[1], device_id=peer, device_id_type=MESH
    )


def neighbours():
    dp, vp = lax.axis_index("dp"), lax.axis_index("vp")
    core = vp + 1 - 2 * lax.rem(vp, 2)
    across = lax.rem(vp + 2, 4)
    other = {"dp": 1 - dp, "vp": vp}
    return dp, vp, across, other, {"dp": dp, "vp": core}, {"dp": dp, "vp": across}


def head_kernel(chunks, pay_ref, n_ref, t_ref, row_ref, slot_ref, cnt_ref, land, acc_n, acc_t, n_bf, send, recv):
    dp, vp, across, other, core, cross = neighbours()
    own, wide = pay_ref.shape
    depth = n_ref.shape[1]
    total = 2 * own
    quarter = own // 4
    part = quarter // chunks
    greet([other, core, cross])
    first, to_core, to_cross, relay = [], [], [], []
    for k in range(chunks):
        rows = pl.ds(k * part, part)
        start = pl.multiple_of(vp * quarter + k * part, 8)
        sem = lambda hop: (send.at[hop, k], recv.at[hop, k])
        first.append(remote(pay_ref.at[pl.ds(start, part), :], land.at[vp, rows, :], sem(0), other))
        to_core.append(remote(land.at[vp, rows, :], land.at[vp, rows, :], sem(1), core))
        to_cross.append(remote(land.at[vp, rows, :], land.at[vp, rows, :], sem(2), cross))
        relay.append(remote(land.at[across, rows, :], land.at[across, rows, :], sem(3), core))
    for copy in first:
        copy.start()
    n_bf[...] = pay_ref[:, :depth].astype(jnp.bfloat16)
    mine = pay_ref[:, depth:]
    my_rows = mine.T

    def forward(k):
        if k < chunks:
            first[k].wait_recv()
            to_core[k].start()
            to_cross[k].start()
        if k > 0:
            to_cross[k - 1].wait_recv()
            relay[k - 1].start()

    forward(0)
    c_own = mine[0:1, 2:3]
    c_other = land[vp, 0:1, depth + 2:depth + 3]
    sum_c = c_own + c_other
    tiles = jnp.maximum(jnp.floor((sum_c + (TILE - 1.0)) * (1.0 / TILE)), float(total // TILE // 2))
    span = tiles * TILE
    cnt_ref[...] = jnp.broadcast_to(jnp.where(lax.broadcasted_iota(jnp.int32, cnt_ref.shape, 1) == 0, c_own, c_other), cnt_ref.shape)
    front = lambda rank: rank - 1.0
    back = lambda rank, c: span - c + rank - 1.0

    def places(code, rank, c, is_front):
        at = jnp.where(is_front, front(rank), back(rank, c))
        return jnp.where(code >= 0.0, at, -1.0)

    my_col = places(mine[:, 0:1], mine[:, 1:2], c_own, dp == 0)
    my_row = places(my_rows[0:1, :], my_rows[1:2, :], c_own, dp == 0)
    tile_of = jnp.floor(my_col * (1.0 / TILE))
    mirrored = (tiles - 1.0 - tile_of) * TILE + (my_col - tile_of * TILE)
    slot = jnp.where(my_col < 0.0, -1.0, jnp.where(dp == 0, my_col, mirrored))
    slot_ref[...] = jnp.broadcast_to(slot, slot_ref.shape)

    def pack(j, at_col, at_row, code, last):
        lanes = lax.broadcasted_iota(jnp.int32, (own, TILE), 1).astype(jnp.float32) + float(j * TILE)
        subs = lax.broadcasted_iota(jnp.int32, (TILE, own), 0).astype(jnp.float32) + float(j * TILE)
        hot_t = at_col == lanes
        hot = (at_row == subs).astype(jnp.float32).astype(jnp.bfloat16)
        cut = slice(j * TILE, (j + 1) * TILE)
        labels = jnp.sum(jnp.where(hot_t, code + 1.0, 0.0), axis=0, keepdims=True)
        hot_t = hot_t.astype(jnp.float32).astype(jnp.bfloat16)
        t = lax.dot_general(n_bf[...], hot_t, (((0,), (0,)), ((), ())), preferred_element_type=jnp.float32)
        n = jnp.dot(hot, n_bf[...], preferred_element_type=jnp.float32)
        if not last:
            acc_t[:, cut] = t
            acc_n[cut, :] = n
            row_ref[0:1, cut] = labels
        else:
            t_ref[:, cut] = (acc_t[:, cut] + t).astype(jnp.bfloat16)
            n_ref[cut, :] = (acc_n[cut, :] + n).astype(jnp.bfloat16)
            row_ref[0:1, cut] = row_ref[0:1, cut] + labels - 1.0

    pieces = list(range(total // TILE))
    step = 0
    for k in range(1, chunks + 1):
        forward(k)
        upto = (len(pieces) * k) // chunks
        for j in pieces[step:upto]:
            pack(j, my_col, my_row, mine[:, 0:1], False)
        step = upto
    for k in range(chunks):
        to_core[k].wait_recv()
        relay[k].wait_recv()
    theirs = land[:, :, depth:].reshape(own, wide - depth)
    their_rows = theirs.T
    n_bf[...] = land[:, :, :depth].reshape(own, depth).astype(jnp.bfloat16)
    their_col = places(theirs[:, 0:1], theirs[:, 1:2], c_other, dp == 1)
    their_row = places(their_rows[0:1, :], their_rows[1:2, :], c_other, dp == 1)
    for j in pieces:
        pack(j, their_col, their_row, theirs[:, 0:1], True)
    for copy in first + to_core + to_cross + relay:
        copy.wait_send()


def head_call(pay, depth, chunks=4):
    own, wide = pay.shape
    total = 2 * own
    return pl.pallas_call(
        functools.partial(head_kernel, chunks),
        in_specs=[pl.BlockSpec(memory_space=pltpu.VMEM)],
        out_specs=[pl.BlockSpec(memory_space=pltpu.VMEM)] * 5,
        out_shape=[
            jax.ShapeDtypeStruct((total, depth), jnp.bfloat16),
            jax.ShapeDtypeStruct((depth, total), jnp.bfloat16),
            jax.ShapeDtypeStruct((8, total), jnp.float32),
            jax.ShapeDtypeStruct((own, 128), jnp.float32),
            jax.ShapeDtypeStruct((8, 128), jnp.float32),
        ],
        scratch_shapes=[
            pltpu.VMEM((4, own // 4, wide), jnp.float32),
            pltpu.VMEM((total, depth), jnp.float32),
            pltpu.VMEM((depth, total), jnp.float32),
            pltpu.VMEM((own, depth), jnp.bfloat16),
            pltpu.SemaphoreType.DMA((4, chunks)),
            pltpu.SemaphoreType.DMA((4, chunks)),
        ],
        compiler_params=pltpu.CompilerParams(collective_id=0, has_side_effects=True, vmem_limit_bytes=VMEM),
        name="head",
    )(pay)


def stats_kernel(vocab, ms_ref, row_ref, cnt_ref, lw_ref, w_ref, lab_ref, sum_ref, land, send, recv):
    dp, vp = lax.axis_index("dp"), lax.axis_index("vp")
    peers = [{"dp": dp, "vp": lax.rem(vp + k, 4)} for k in (1, 2, 3)]
    greet(peers)
    copies = [remote(ms_ref, land.at[vp], (send.at[k], recv.at[k]), peer) for k, peer in enumerate(peers)]
    for copy in copies:
        copy.start()
    land[vp] = ms_ref[...]
    labels = row_ref[0:1, :]
    live = labels >= 0.0
    weight = LOGIT_SCALE / jnp.sum(cnt_ref[0:1, 0:2], axis=1, keepdims=True)
    rel = labels - (vp * vocab).astype(jnp.float32)
    lab_ref[...] = jnp.where(live & (rel < float(vocab)), rel, -1.0).astype(jnp.int32)
    w_ref[...] = jnp.where(live, weight, 0.0)
    for copy in copies:
        copy.wait()
    best = jnp.max(land[:, 0:1, :], axis=0)
    total = sum(land[k, 1:2, :] * jnp.exp2(land[k, 0:1, :] - best) for k in range(4))
    lse = best + jnp.log(total) * LOG2E
    lw_ref[...] = jnp.where(live, lse - jnp.log(weight) * LOG2E, -NEG)
    sum_ref[...] = jnp.broadcast_to(jnp.sum(jnp.where(live, lse, 0.0), axis=1, keepdims=True), sum_ref.shape)


def stats_call(ms, row, cnt, vocab):
    total = ms.shape[1]
    line = lambda t: jax.ShapeDtypeStruct((1, total), t)
    return pl.pallas_call(
        functools.partial(stats_kernel, vocab),
        in_specs=[pl.BlockSpec(memory_space=pltpu.VMEM)] * 3,
        out_specs=[pl.BlockSpec(memory_space=pltpu.VMEM)] * 4,
        out_shape=[line(jnp.float32), line(jnp.float32), line(jnp.int32), jax.ShapeDtypeStruct((8, 128), jnp.float32)],
        scratch_shapes=[pltpu.VMEM((4, 8, total), jnp.float32), pltpu.SemaphoreType.DMA((3,)), pltpu.SemaphoreType.DMA((3,))],
        compiler_params=pltpu.CompilerParams(collective_id=1, has_side_effects=True),
        name="stats",
    )(ms, row, cnt)


def tail_kernel(chunks, dn_ref, lz_ref, h_ref, gain_ref, slot_ref, w_ref, sum_ref, cnt_ref, dh_ref, dg_ref, loss_ref,
                land1, part, land2, full, lz_land, gain_out, gain_in, send, recv, small_send, small_recv):
    dp, vp, across, other, core, cross = neighbours()
    c = lax.rem(vp, 2)
    halves, hrows, slots = dn_ref.shape
    depth = halves * hrows
    rows_k = hrows // chunks
    peers = [{"dp": dp, "vp": lax.rem(vp + k, 4)} for k in (1, 2, 3)]
    greet(peers + [other])
    lz_copies = [remote(lz_ref, lz_land.at[vp], (small_send.at[k], small_recv.at[k]), peer) for k, peer in enumerate(peers)]
    swap, over, back = [], [], []
    for k in range(chunks):
        rows = pl.ds(k * rows_k, rows_k)
        sem = lambda hop: (send.at[hop, k], recv.at[hop, k])
        swap.append(remote(dn_ref.at[1 - c, rows, :], land1.at[rows, :], sem(0), core))
        over.append(remote(part.at[rows, :], land2.at[rows, :], sem(1), cross))
        back.append(remote(full.at[c, rows, :], full.at[c, rows, :], sem(2), core))
    for copy in swap:
        copy.start()
    for k in range(chunks):
        rows = pl.ds(k * rows_k, rows_k)
        swap[k].wait_recv()
        part[rows, :] = dn_ref[c, rows, :] + land1[rows, :]
        over[k].start()
    for copy in lz_copies:
        copy.start()
    lz_land[vp] = lz_ref[...]
    tokens = h_ref.shape[0]
    pick = (lax.broadcasted_iota(jnp.int32, (tokens, slots), 1).astype(jnp.float32) == slot_ref[:, 0:1]).astype(jnp.float32).astype(jnp.bfloat16)
    h = lax.dot_general(h_ref[...], pick, (((0,), (0,)), ((), ())), preferred_element_type=jnp.float32)
    centered = h - jnp.mean(h, axis=0, keepdims=True)
    inv = lax.rsqrt(jnp.mean(centered * centered, axis=0, keepdims=True) + EPS)
    xhat = centered * inv
    for k in range(chunks):
        rows = pl.ds(k * rows_k, rows_k)
        over[k].wait_recv()
        full[c, rows, :] = part[rows, :] + land2[rows, :]
        back[k].start()
    for copy in lz_copies:
        copy.wait()
    for copy in back:
        copy.wait_recv()
    dn = full[...].reshape(depth, slots)
    prod = dn * xhat
    lanes = sum(prod[:, i * 128:(i + 1) * 128] for i in range(slots // 128))
    gain_out[...] = jnp.broadcast_to(jnp.sum(lanes.T, axis=0, keepdims=True), gain_out.shape)
    share = remote(gain_out, gain_in, (small_send.at[3], small_recv.at[3]), other)
    share.start()
    a = dn * gain_ref[...]
    one = jnp.mean(a, axis=0, keepdims=True)
    two = jnp.mean(a * xhat, axis=0, keepdims=True)
    dh = (inv * (a - one - xhat * two)).astype(jnp.bfloat16)
    dh_ref[...] = lax.dot_general(pick, dh, (((1,), (1,)), ((), ())), preferred_element_type=jnp.float32).astype(jnp.bfloat16)
    live = w_ref[...] > 0.0
    label_sum = jnp.zeros((1, 1), jnp.float32)
    for k in range(4):
        line = jnp.sum(lz_land[k], axis=0, keepdims=True)
        label_sum = label_sum + jnp.sum(jnp.where(live, line, 0.0), axis=1, keepdims=True)
    count = jnp.sum(cnt_ref[0:1, 0:2], axis=1, keepdims=True)
    loss = (sum_ref[0:1, 0:1] - label_sum) * LN2 / count
    loss_ref[...] = jnp.broadcast_to(loss, loss_ref.shape)
    share.wait()
    dg_ref[...] = gain_out[...] + gain_in[...]
    for copy in swap + over + back:
        copy.wait_send()


def tail_call(dn, lz, h, gain, slot, w, lse_sum, cnt, chunks=4):
    tokens, depth = h.shape
    slots = dn.shape[1]
    half = depth // 2
    return pl.pallas_call(
        functools.partial(tail_kernel, chunks),
        in_specs=[pl.BlockSpec(memory_space=pltpu.VMEM)] * 8,
        out_specs=[pl.BlockSpec(memory_space=pltpu.VMEM)] * 3,
        out_shape=[
            jax.ShapeDtypeStruct((tokens, depth), jnp.bfloat16),
            jax.ShapeDtypeStruct((8, depth), jnp.float32),
            jax.ShapeDtypeStruct((8, 128), jnp.float32),
        ],
        scratch_shapes=[
            pltpu.VMEM((half, slots), jnp.float32),
            pltpu.VMEM((half, slots), jnp.float32),
            pltpu.VMEM((half, slots), jnp.float32),
            pltpu.VMEM((2, half, slots), jnp.float32),
            pltpu.VMEM((4, 8, lz.shape[1]), jnp.float32),
            pltpu.VMEM((8, depth), jnp.float32),
            pltpu.VMEM((8, depth), jnp.float32),
            pltpu.SemaphoreType.DMA((3, chunks)),
            pltpu.SemaphoreType.DMA((3, chunks)),
            pltpu.SemaphoreType.DMA((4,)),
            pltpu.SemaphoreType.DMA((4,)),
        ],
        compiler_params=pltpu.CompilerParams(collective_id=2, has_side_effects=True, vmem_limit_bytes=VMEM),
        name="tail",
    )(dn.reshape(2, half, slots), lz, h, gain.reshape(depth, 1), slot, w, lse_sum, cnt)


def solution(mesh):
    def local_step(hidden, norm_gain, emb_table, labels, tok_mask):
        rows, seq_len, depth = hidden.shape
        vocab_local = emb_table.shape[0]
        own = rows * seq_len
        flat = hidden.reshape(own, depth)
        dp = lax.axis_index("dp")
        max_tiles = 2 * own // TILE

        mask = tok_mask.reshape(own, 1)
        ranks = jnp.cumsum(mask, axis=0)
        code = jnp.where(mask > 0, labels.reshape(own, 1).astype(jnp.float32), -1.0)
        lane = jnp.arange(128)[None, :]
        meta = jnp.where(lane == 0, code, jnp.where(lane == 1, ranks, ranks[own - 1:own]))
        values = flat.astype(jnp.float32)
        mu = jnp.mean(values, axis=-1, keepdims=True)
        centered = values - mu
        var = jnp.mean(centered * centered, axis=-1, keepdims=True)
        normed = (norm_gain * (centered * lax.rsqrt(var + EPS))).astype(jnp.bfloat16)
        pay = jnp.concatenate([normed.astype(jnp.float32), meta], axis=1)
        packed, packed_t, line, slot, cnt = head_call(pay, depth)

        n_own, n_other = cnt[0, 0].astype(jnp.int32), cnt[0, 1].astype(jnp.int32)
        tiles = (n_own + n_other + TILE - 1) // TILE
        which = jnp.clip(tiles - max_tiles // 2, 0, max_tiles - max_tiles // 2)
        variants = range(max_tiles // 2, max_tiles + 1)
        z, ms = lax.switch(which, [functools.partial(logits_call, nt, 1536 if nt < 6 else 1280, 128) for nt in variants], emb_table, packed_t)
        lw, w, rel_labels, lse_sum = stats_call(ms, line, cnt, vocab_local)
        info = jnp.stack([(n_own + TILE - 1) // TILE, dp]).astype(jnp.int32)
        d_table, dn_t, lz = lax.switch(
            which,
            [functools.partial(grad_call, nt, 1536 if nt < 6 else 1280, 256, own // TILE) for nt in variants],
            info, z, emb_table, packed, lw, w, rel_labels,
        )
        d_tokens, d_gain, loss = tail_call(dn_t, lz, flat, norm_gain, slot, w, lse_sum, cnt)
        return loss[0, 0], d_table, d_tokens.reshape(rows, seq_len, depth), d_gain[0]

    return jax.shard_map(
        local_step,
        mesh=mesh,
        in_specs=(P("dp", None, None), P(None), P("vp", None), P("dp", None), P("dp", None)),
        out_specs=(P(), P("vp", None), P("dp", None, None), P(None)),
        check_vma=False,
    )
```

```python
import functools

import jax
import jax.numpy as jnp
from jax import lax
from jax.experimental import pallas as pl
from jax.experimental.pallas import tpu as pltpu
from jax.sharding import PartitionSpec as P

LOGIT_SCALE = 0.0625
EPS = 1e-5
LOG2E = 1.4426950408889634
LN2 = 0.6931471805599453
NEG = -1e30
TILE = 256
VMEM = 63 * 2**20


def logits_kernel(vocab, bv, rc, e_ref, nt_ref, z_ref, ms_ref, m_ref, s_ref):
    i = pl.program_id(0)

    @pl.when(i == 0)
    def _():
        m_ref[...] = jnp.full(m_ref.shape, NEG, jnp.float32)
        s_ref[...] = jnp.zeros(s_ref.shape, jnp.float32)

    width = nt_ref.shape[1]
    limit = vocab - i * bv
    for r in range(0, bv, rc):
        z = jnp.dot(e_ref[pl.ds(r, rc), :], nt_ref[...], preferred_element_type=jnp.float32)
        rows = lax.broadcasted_iota(jnp.int32, (rc, width), 0) + r
        z = jnp.where(rows < limit, z * (LOGIT_SCALE * LOG2E), NEG)
        z_ref[pl.ds(r, rc), :] = z
        groups = z.reshape(rc // 8, 8, width)
        old = m_ref[...]
        new = jnp.maximum(old, jnp.max(groups, axis=0))
        s_ref[...] = s_ref[...] * jnp.exp2(old - new) + jnp.sum(jnp.exp2(groups - new[None]), axis=0)
        m_ref[...] = new

    @pl.when(i == pl.num_programs(0) - 1)
    def _():
        best = jnp.max(m_ref[...], axis=0, keepdims=True)
        ms_ref[0:1, :] = best
        ms_ref[1:2, :] = jnp.sum(s_ref[...] * jnp.exp2(m_ref[...] - best), axis=0, keepdims=True)


def logits_call(nt, bv, rc, z_rows, table, normed_t):
    vocab, depth = table.shape
    steps = pl.cdiv(vocab, bv)
    width = nt * TILE
    full = normed_t.shape[1]
    fixed = lambda i: (0, 0)
    return pl.pallas_call(
        functools.partial(logits_kernel, vocab, bv, rc),
        grid=(steps,),
        in_specs=[pl.BlockSpec((bv, depth), lambda i: (i, 0)), pl.BlockSpec((depth, width), fixed)],
        out_specs=[pl.BlockSpec((bv, width), lambda i: (i, 0)), pl.BlockSpec((8, width), fixed)],
        out_shape=[jax.ShapeDtypeStruct((z_rows, full), jnp.float32), jax.ShapeDtypeStruct((8, full), jnp.float32)],
        scratch_shapes=[pltpu.VMEM((8, width), jnp.float32), pltpu.VMEM((8, width), jnp.float32)],
        compiler_params=pltpu.CompilerParams(dimension_semantics=("arbitrary",), vmem_limit_bytes=VMEM),
        name=f"logits_{nt}",
    )(table, normed_t)


def grad_kernel(vocab, bv, rc, nt, own, info_ref, z_ref, e_ref, n_ref, lw_ref, w_ref, lab_ref, dt_ref, dn_ref, lz_ref, dz_ref, et_ref):
    i = pl.program_id(0)

    @pl.when(i == 0)
    def _():
        dn_ref[...] = jnp.zeros(dn_ref.shape, jnp.float32)
        lz_ref[...] = jnp.zeros(lz_ref.shape, jnp.float32)

    width = nt * TILE
    limit = vocab - i * bv
    labels = lab_ref[...] - i * bv
    lw = lw_ref[...]
    w = w_ref[...]
    for r in range(0, bv, rc):
        z = z_ref[pl.ds(r, rc), :]
        hit = lax.broadcasted_iota(jnp.int32, (rc, width), 0) + r == labels
        dz = (jnp.exp2(z - lw) - jnp.where(hit, w, 0.0)).astype(jnp.bfloat16)
        lz_ref[...] += jnp.sum(jnp.where(hit, z, 0.0).reshape(rc // 8, 8, width), axis=0)
        dz_ref[pl.ds(r, rc), :] = dz
        dt_ref[pl.ds(r, rc), :] = jnp.dot(dz, n_ref[...], preferred_element_type=jnp.float32)
        rows = lax.broadcasted_iota(jnp.int32, (rc, e_ref.shape[1]), 0) + r
        et_ref[:, pl.ds(r, rc)] = jnp.where(rows < limit, e_ref[pl.ds(r, rc), :], jnp.zeros((), jnp.bfloat16)).T
    for k in range(2, own + 1):
        @pl.when(info_ref[0] == k)
        def _():
            start = jnp.where(info_ref[1] == 0, 0, nt - k)
            cols = pl.ds(pl.multiple_of(start * TILE, TILE), k * TILE)
            dn_ref[:, :k * TILE] += jnp.dot(et_ref[...], dz_ref[:, cols], preferred_element_type=jnp.float32)


def grad_call(nt, bv, rc, own_max, info, z, table, normed, lw, w, labels):
    vocab, depth = table.shape
    steps = pl.cdiv(vocab, bv)
    width = nt * TILE
    full = normed.shape[0]
    own = min(nt, own_max)
    fixed = lambda i, *_: (0, 0)
    step = lambda i, *_: (i, 0)
    return pl.pallas_call(
        functools.partial(grad_kernel, vocab, bv, rc, nt, own),
        grid_spec=pltpu.PrefetchScalarGridSpec(
            num_scalar_prefetch=1,
            grid=(steps,),
            in_specs=[
                pl.BlockSpec((bv, width), step),
                pl.BlockSpec((bv, depth), step),
                pl.BlockSpec((width, depth), fixed),
                pl.BlockSpec((1, width), fixed),
                pl.BlockSpec((1, width), fixed),
                pl.BlockSpec((1, width), fixed),
            ],
            out_specs=[pl.BlockSpec((bv, depth), step), pl.BlockSpec((depth, own_max * TILE), fixed), pl.BlockSpec((8, width), fixed)],
            scratch_shapes=[pltpu.VMEM((bv, width), jnp.bfloat16), pltpu.VMEM((depth, bv), jnp.bfloat16)],
        ),
        out_shape=[
            jax.ShapeDtypeStruct((vocab, depth), jnp.float32),
            jax.ShapeDtypeStruct((depth, own_max * TILE), jnp.float32),
            jax.ShapeDtypeStruct((8, full), jnp.float32),
        ],
        compiler_params=pltpu.CompilerParams(dimension_semantics=("arbitrary",), vmem_limit_bytes=VMEM),
        name=f"grads_{nt}",
    )(info, z, table, normed, lw, w, labels)


MESH = pl.DeviceIdType.MESH


def greet(peers):
    barrier = pltpu.get_barrier_semaphore()
    for peer in peers:
        pl.semaphore_signal(barrier, inc=1, device_id=peer, device_id_type=MESH)
    pl.semaphore_wait(barrier, len(peers))


def remote(src, dst, sems, peer):
    return pltpu.make_async_remote_copy(
        src_ref=src, dst_ref=dst, send_sem=sems[0], recv_sem=sems[1], device_id=peer, device_id_type=MESH
    )


def neighbours():
    dp, vp = lax.axis_index("dp"), lax.axis_index("vp")
    core = vp + 1 - 2 * lax.rem(vp, 2)
    across = lax.rem(vp + 2, 4)
    other = {"dp": 1 - dp, "vp": vp}
    return dp, vp, across, other, {"dp": dp, "vp": core}, {"dp": dp, "vp": across}


def head_kernel(chunks, least, h_ref, gain_ref, marks_ref, n_ref, t_ref, row_ref, slot_ref, info_ref,
                land, pay, meta, their_meta, acc_n, acc_t, n_bf, send, recv, meta_send, meta_recv):
    dp, vp, across, other, core, cross = neighbours()
    own, depth = h_ref.shape
    total = 2 * own
    quarter = own // 4
    part = quarter // chunks
    barrier = pltpu.get_barrier_semaphore()
    for peer in (other, core, cross):
        pl.semaphore_signal(barrier, inc=1, device_id=peer, device_id_type=MESH)
    values = h_ref[...].astype(jnp.float32)
    centered = values - jnp.mean(values, axis=1, keepdims=True)
    var = jnp.mean(centered * centered, axis=1, keepdims=True)
    n_bf[...] = (gain_ref[...] * (centered * lax.rsqrt(var + EPS))).astype(jnp.bfloat16)
    pay[...] = n_bf[pl.ds(pl.multiple_of(vp * quarter, 16), quarter), :].astype(jnp.float32)
    flat = lambda at: jnp.concatenate([marks_ref[at + i:at + i + 1, :] for i in range(own // marks_ref.shape[1])], axis=1)
    mask = flat(0)
    code = jnp.where(mask > 0.0, flat(8), -1.0)
    upper = lax.broadcasted_iota(jnp.int32, (own, own), 0) <= lax.broadcasted_iota(jnp.int32, (own, own), 1)
    mask8 = jnp.broadcast_to(mask, (8, own)).astype(jnp.bfloat16)
    ranks = jnp.dot(mask8, upper.astype(jnp.float32).astype(jnp.bfloat16), preferred_element_type=jnp.float32)
    count = jnp.broadcast_to(jnp.sum(mask, axis=1, keepdims=True), (8, own))
    line = lax.broadcasted_iota(jnp.int32, (8, own), 0)
    meta[...] = jnp.where(line == 0, code, jnp.where(line == 1, ranks, count))
    pl.semaphore_wait(barrier, 3)
    swap = remote(meta, their_meta, (meta_send, meta_recv), other)
    swap.start()

    def copies(k):
        rows = pl.ds(pl.multiple_of(k * part, 8), part)
        sem = lambda hop: (send.at[hop, k], recv.at[hop, k])
        mine, theirs = land.at[vp, rows, :], land.at[across, rows, :]
        return (
            remote(pay.at[rows, :], mine, sem(0), other),
            remote(mine, mine, sem(1), core),
            remote(mine, mine, sem(2), cross),
            remote(theirs, theirs, sem(3), core),
        )

    for k in range(chunks):
        copies(k)[0].start()

    swap.wait_recv()
    c_own, c_other = meta[2:3, 0:1], their_meta[2:3, 0:1]
    ceil_tiles = lambda c: jnp.floor((c + (TILE - 1.0)) * (1.0 / TILE))
    tiles = jnp.maximum(ceil_tiles(c_own + c_other), float(least))
    own_tiles = jnp.maximum(ceil_tiles(c_own), 2.0)
    lane = lax.broadcasted_iota(jnp.int32, info_ref.shape, 1)
    info = jnp.where(lane == 0, own_tiles, jnp.where(lane == 1, dp.astype(jnp.float32), tiles - float(least)))
    info_ref[...] = info.astype(jnp.int32)

    def places(block, is_front):
        back = tiles * TILE - block[2:3, :]
        at = jnp.where(is_front, 0.0, back) + block[1:2, :] - 1.0
        at = jnp.where(block[0:1, :] >= 0.0, at, -1.0)
        both = jnp.where(line == 0, at, jnp.broadcast_to(block[0:1, :], (8, own)) + 1.0)
        return at, both.T

    my_row, my_cols = places(meta, dp == 0)
    my_col = my_cols[:, 0:1]
    base = jnp.where(dp == 0, 0.0, (tiles - own_tiles) * TILE)
    slot_ref[...] = jnp.broadcast_to(jnp.where(my_col < 0.0, -1.0, my_col - base), slot_ref.shape)

    def pack(j, at_col, at_row, code_col, last):
        start = pl.multiple_of(j * TILE, TILE)
        offset = (j * TILE).astype(jnp.float32)
        lanes = lax.broadcasted_iota(jnp.int32, (own, TILE), 1).astype(jnp.float32) + offset
        subs = lax.broadcasted_iota(jnp.int32, (TILE, own), 0).astype(jnp.float32) + offset
        hot_t = at_col == lanes
        hot = (at_row == subs).astype(jnp.float32).astype(jnp.bfloat16)
        cut = pl.ds(start, TILE)
        labels = jnp.sum(jnp.where(hot_t, code_col, 0.0), axis=0, keepdims=True)
        hot_t = hot_t.astype(jnp.float32).astype(jnp.bfloat16)
        t = lax.dot_general(n_bf[...], hot_t, (((0,), (0,)), ((), ())), preferred_element_type=jnp.float32)
        n = jnp.dot(hot, n_bf[...], preferred_element_type=jnp.float32)
        if not last:
            acc_t[:, cut] = t
            acc_n[cut, :] = n
            row_ref[0:1, cut] = labels
        else:
            t_ref[:, cut] = (acc_t[:, cut] + t).astype(jnp.bfloat16)
            n_ref[cut, :] = (acc_n[cut, :] + n).astype(jnp.bfloat16)
            row_ref[0:1, cut] = row_ref[0:1, cut] + labels - 1.0

    @pl.loop(0, chunks)
    def _(k):
        first, to_core, to_cross, _ = copies(k)
        first.wait_recv()
        to_core.start()
        to_cross.start()

        @pl.when(k > 0)
        def _():
            _, _, arrived, relay = copies(k - 1)
            arrived.wait_recv()
            relay.start()

        pack(k, my_cols[:, 0:1], my_row, my_cols[:, 1:2], False)

    _, _, arrived, relay = copies(chunks - 1)
    arrived.wait_recv()
    relay.start()
    their_row, their_cols = places(their_meta, dp == 1)
    for k in range(chunks):
        _, to_core, _, relay = copies(k)
        to_core.wait_recv()
        relay.wait_recv()
    n_bf[...] = land[...].reshape(own, depth).astype(jnp.bfloat16)

    @pl.loop(0, total // TILE)
    def _(j):
        pack(j, their_cols[:, 0:1], their_row, their_cols[:, 1:2], True)

    swap.wait_send()
    for k in range(chunks):
        for copy in copies(k):
            copy.wait_send()


def head_call(h, gain, marks, least):
    own, depth = h.shape
    total = 2 * own
    chunks = total // TILE
    return pl.pallas_call(
        functools.partial(head_kernel, chunks, least),
        in_specs=[pl.BlockSpec(memory_space=pltpu.VMEM)] * 3,
        out_specs=[pl.BlockSpec(memory_space=pltpu.VMEM)] * 5,
        out_shape=[
            jax.ShapeDtypeStruct((total, depth), jnp.bfloat16),
            jax.ShapeDtypeStruct((depth, total), jnp.bfloat16),
            jax.ShapeDtypeStruct((8, total), jnp.float32),
            jax.ShapeDtypeStruct((own, 128), jnp.float32),
            jax.ShapeDtypeStruct((8, 128), jnp.int32),
        ],
        scratch_shapes=[
            pltpu.VMEM((4, own // 4, depth), jnp.float32),
            pltpu.VMEM((own // 4, depth), jnp.float32),
            pltpu.VMEM((8, own), jnp.float32),
            pltpu.VMEM((8, own), jnp.float32),
            pltpu.VMEM((total, depth), jnp.float32),
            pltpu.VMEM((depth, total), jnp.float32),
            pltpu.VMEM((own, depth), jnp.bfloat16),
            pltpu.SemaphoreType.DMA((4, chunks)),
            pltpu.SemaphoreType.DMA((4, chunks)),
            pltpu.SemaphoreType.DMA,
            pltpu.SemaphoreType.DMA,
        ],
        compiler_params=pltpu.CompilerParams(collective_id=0, has_side_effects=True, vmem_limit_bytes=VMEM),
        name="head",
    )(h, gain.reshape(1, depth), marks)


def stats_kernel(vocab, ms_ref, row_ref, lw_ref, w_ref, lab_ref, sum_ref, land, send, recv):
    dp, vp = lax.axis_index("dp"), lax.axis_index("vp")
    peers = [{"dp": dp, "vp": lax.rem(vp + k, 4)} for k in (1, 2, 3)]
    greet(peers)
    copies = [remote(ms_ref, land.at[vp], (send.at[k], recv.at[k]), peer) for k, peer in enumerate(peers)]
    for copy in copies:
        copy.start()
    land[vp] = ms_ref[...]
    labels = row_ref[0:1, :]
    live = labels >= 0.0
    count = jnp.sum(jnp.where(live, 1.0, 0.0), axis=1, keepdims=True)
    weight = LOGIT_SCALE / count
    rel = labels - (vp * vocab).astype(jnp.float32)
    lab_ref[...] = jnp.where(live & (rel < float(vocab)), rel, -1.0).astype(jnp.int32)
    w_ref[...] = jnp.where(live, weight, 0.0)
    for copy in copies:
        copy.wait()
    best = jnp.max(land[:, 0:1, :], axis=0)
    total = sum(land[k, 1:2, :] * jnp.exp2(land[k, 0:1, :] - best) for k in range(4))
    lse = best + jnp.log(total) * LOG2E
    lw_ref[...] = jnp.where(live, lse - jnp.log(weight) * LOG2E, -NEG)
    lse_sum = jnp.sum(jnp.where(live, lse, 0.0), axis=1, keepdims=True)
    sum_ref[...] = jnp.where(lax.broadcasted_iota(jnp.int32, sum_ref.shape, 1) == 0, lse_sum, count)


def stats_call(ms, row, vocab):
    total = ms.shape[1]
    line = lambda t: jax.ShapeDtypeStruct((1, total), t)
    return pl.pallas_call(
        functools.partial(stats_kernel, vocab),
        in_specs=[pl.BlockSpec(memory_space=pltpu.VMEM)] * 2,
        out_specs=[pl.BlockSpec(memory_space=pltpu.VMEM)] * 4,
        out_shape=[line(jnp.float32), line(jnp.float32), line(jnp.int32), jax.ShapeDtypeStruct((8, 128), jnp.float32)],
        scratch_shapes=[pltpu.VMEM((4, 8, total), jnp.float32), pltpu.SemaphoreType.DMA((3,)), pltpu.SemaphoreType.DMA((3,))],
        compiler_params=pltpu.CompilerParams(collective_id=1, has_side_effects=True),
        name="stats",
    )(ms, row)


def tail_kernel(chunks, dn_ref, lz_ref, h_ref, gain_ref, slot_ref, w_ref, sum_ref, dh_ref, dg_ref, loss_ref,
                land1, part, land2, full, lz_land, gain_out, gain_in, send, recv, small_send, small_recv):
    dp, vp, across, other, core, cross = neighbours()
    c = lax.rem(vp, 2)
    halves, hrows, slots = dn_ref.shape
    depth = halves * hrows
    rows_k = hrows // chunks
    peers = [{"dp": dp, "vp": lax.rem(vp + k, 4)} for k in (1, 2, 3)]
    greet(peers + [other])
    lz_copies = [remote(lz_ref, lz_land.at[vp], (small_send.at[k], small_recv.at[k]), peer) for k, peer in enumerate(peers)]
    swap, over, back = [], [], []
    for k in range(chunks):
        rows = pl.ds(k * rows_k, rows_k)
        sem = lambda hop: (send.at[hop, k], recv.at[hop, k])
        swap.append(remote(dn_ref.at[1 - c, rows, :], land1.at[rows, :], sem(0), core))
        over.append(remote(part.at[rows, :], land2.at[rows, :], sem(1), cross))
        back.append(remote(full.at[c, rows, :], full.at[c, rows, :], sem(2), core))
    for copy in swap:
        copy.start()
    for k in range(chunks):
        rows = pl.ds(k * rows_k, rows_k)
        swap[k].wait_recv()
        part[rows, :] = dn_ref[c, rows, :] + land1[rows, :]
        over[k].start()
    for copy in lz_copies:
        copy.start()
    lz_land[vp] = lz_ref[...]
    tokens = h_ref.shape[0]
    pick = (lax.broadcasted_iota(jnp.int32, (tokens, slots), 1).astype(jnp.float32) == slot_ref[:, 0:1]).astype(jnp.float32).astype(jnp.bfloat16)
    h = lax.dot_general(h_ref[...], pick, (((0,), (0,)), ((), ())), preferred_element_type=jnp.float32)
    centered = h - jnp.mean(h, axis=0, keepdims=True)
    inv = lax.rsqrt(jnp.mean(centered * centered, axis=0, keepdims=True) + EPS)
    xhat = centered * inv
    for k in range(chunks):
        rows = pl.ds(k * rows_k, rows_k)
        over[k].wait_recv()
        full[c, rows, :] = part[rows, :] + land2[rows, :]
        back[k].start()
    for copy in lz_copies:
        copy.wait()
    for copy in back:
        copy.wait_recv()
    dn = full[...].reshape(depth, slots)
    prod = dn * xhat
    lanes = sum(prod[:, i * 128:(i + 1) * 128] for i in range(slots // 128))
    gain_out[...] = jnp.broadcast_to(jnp.sum(lanes.T, axis=0, keepdims=True), gain_out.shape)
    share = remote(gain_out, gain_in, (small_send.at[3], small_recv.at[3]), other)
    share.start()
    a = dn * jnp.broadcast_to(gain_ref[...], (8, depth)).T[:, 0:1]
    one = jnp.mean(a, axis=0, keepdims=True)
    two = jnp.mean(a * xhat, axis=0, keepdims=True)
    dh = (inv * (a - one - xhat * two)).astype(jnp.bfloat16)
    dh_ref[...] = lax.dot_general(pick, dh, (((1,), (1,)), ((), ())), preferred_element_type=jnp.float32).astype(jnp.bfloat16)
    live = w_ref[...] > 0.0
    label_sum = jnp.zeros((1, 1), jnp.float32)
    for k in range(4):
        line = jnp.sum(lz_land[k], axis=0, keepdims=True)
        label_sum = label_sum + jnp.sum(jnp.where(live, line, 0.0), axis=1, keepdims=True)
    loss = (sum_ref[0:1, 0:1] - label_sum) * LN2 / sum_ref[0:1, 1:2]
    loss_ref[...] = jnp.broadcast_to(loss, loss_ref.shape)
    share.wait()
    dg_ref[...] = gain_out[...] + gain_in[...]
    for copy in swap + over + back:
        copy.wait_send()


def tail_call(dn, lz, h, gain, slot, w, sums, chunks=4):
    tokens, depth = h.shape
    slots = dn.shape[1]
    half = depth // 2
    return pl.pallas_call(
        functools.partial(tail_kernel, chunks),
        in_specs=[pl.BlockSpec(memory_space=pltpu.VMEM)] * 7,
        out_specs=[pl.BlockSpec(memory_space=pltpu.VMEM)] * 3,
        out_shape=[
            jax.ShapeDtypeStruct((tokens, depth), jnp.bfloat16),
            jax.ShapeDtypeStruct((8, depth), jnp.float32),
            jax.ShapeDtypeStruct((8, 128), jnp.float32),
        ],
        scratch_shapes=[
            pltpu.VMEM((half, slots), jnp.float32),
            pltpu.VMEM((half, slots), jnp.float32),
            pltpu.VMEM((half, slots), jnp.float32),
            pltpu.VMEM((2, half, slots), jnp.float32),
            pltpu.VMEM((4, 8, lz.shape[1]), jnp.float32),
            pltpu.VMEM((8, depth), jnp.float32),
            pltpu.VMEM((8, depth), jnp.float32),
            pltpu.SemaphoreType.DMA((3, chunks)),
            pltpu.SemaphoreType.DMA((3, chunks)),
            pltpu.SemaphoreType.DMA((4,)),
            pltpu.SemaphoreType.DMA((4,)),
        ],
        compiler_params=pltpu.CompilerParams(collective_id=2, has_side_effects=True, vmem_limit_bytes=VMEM),
        name="tail",
    )(dn.reshape(2, half, slots), lz, h, gain.reshape(1, depth), slot, w, sums)


def solution(mesh):
    def local_step(hidden, norm_gain, emb_table, labels, tok_mask):
        rows, seq_len, depth = hidden.shape
        vocab_local = emb_table.shape[0]
        own = rows * seq_len
        flat = hidden.reshape(own, depth)
        pad = ((0, 8 - rows), (0, 0))
        marks = jnp.concatenate([jnp.pad(tok_mask, pad), jnp.pad(labels.astype(jnp.float32), pad)], axis=0)
        most = 2 * own // TILE
        variants = {nt: (1536 if nt < most else 256) for nt in range(2 * most // 3, most + 1)}
        z_rows = max(bv * pl.cdiv(vocab_local, bv) for bv in variants.values())
        packed, packed_t, line, slot, info = head_call(flat, norm_gain, marks, min(variants))
        which = jnp.clip(info[0, 2], 0, len(variants) - 1)
        z, ms = lax.switch(which, [functools.partial(logits_call, nt, bv, 128, z_rows) for nt, bv in variants.items()], emb_table, packed_t)
        lw, w, rel_labels, sums = stats_call(ms, line, vocab_local)
        d_table, dn_t, lz = lax.switch(
            which,
            [functools.partial(grad_call, nt, bv, 256, own // TILE) for nt, bv in variants.items()],
            info[0, :2], z, emb_table, packed, lw, w, rel_labels,
        )
        d_tokens, d_gain, loss = tail_call(dn_t, lz, flat, norm_gain, slot, w, sums)
        return loss[0, 0], d_table, d_tokens.reshape(rows, seq_len, depth), d_gain[0]

    return jax.shard_map(
        local_step,
        mesh=mesh,
        in_specs=(P("dp", None, None), P(None), P("vp", None), P("dp", None), P("dp", None)),
        out_specs=(P(), P("vp", None), P("dp", None, None), P(None)),
        check_vma=False,
    )
```

```python
import functools

import jax
import jax.numpy as jnp
from jax import lax
from jax.experimental import pallas as pl
from jax.experimental.pallas import tpu as pltpu
from jax.sharding import PartitionSpec as P

LOGIT_SCALE = 0.0625
EPS = 1e-5
LOG2E = 1.4426950408889634
LN2 = 0.6931471805599453
NEG = -1e30
TILE = 256
VMEM = 63 * 2**20


def logits_kernel(vocab, bv, rc, e_ref, nt_ref, z_ref, ms_ref, m_ref, s_ref):
    i = pl.program_id(0)

    @pl.when(i == 0)
    def _():
        m_ref[...] = jnp.full(m_ref.shape, NEG, jnp.float32)
        s_ref[...] = jnp.zeros(s_ref.shape, jnp.float32)

    width = nt_ref.shape[1]
    limit = vocab - i * bv
    for r in range(0, bv, rc):
        z = jnp.dot(e_ref[pl.ds(r, rc), :], nt_ref[...], preferred_element_type=jnp.float32)
        rows = lax.broadcasted_iota(jnp.int32, (rc, width), 0) + r
        z = jnp.where(rows < limit, z * (LOGIT_SCALE * LOG2E), NEG)
        z_ref[pl.ds(r, rc), :] = z
        groups = z.reshape(rc // 8, 8, width)
        old = m_ref[...]
        new = jnp.maximum(old, jnp.max(groups, axis=0))
        s_ref[...] = s_ref[...] * jnp.exp2(old - new) + jnp.sum(jnp.exp2(groups - new[None]), axis=0)
        m_ref[...] = new

    @pl.when(i == pl.num_programs(0) - 1)
    def _():
        best = jnp.max(m_ref[...], axis=0, keepdims=True)
        ms_ref[0:1, :] = best
        ms_ref[1:2, :] = jnp.sum(s_ref[...] * jnp.exp2(m_ref[...] - best), axis=0, keepdims=True)


def logits_call(nt, bv, rc, z_rows, table, normed_t):
    vocab, depth = table.shape
    steps = pl.cdiv(vocab, bv)
    width = nt * TILE
    full = normed_t.shape[1]
    fixed = lambda i: (0, 0)
    return pl.pallas_call(
        functools.partial(logits_kernel, vocab, bv, rc),
        grid=(steps,),
        in_specs=[pl.BlockSpec((bv, depth), lambda i: (i, 0)), pl.BlockSpec((depth, width), fixed)],
        out_specs=[pl.BlockSpec((bv, width), lambda i: (i, 0)), pl.BlockSpec((8, width), fixed)],
        out_shape=[jax.ShapeDtypeStruct((z_rows, full), jnp.float32), jax.ShapeDtypeStruct((8, full), jnp.float32)],
        scratch_shapes=[pltpu.VMEM((8, width), jnp.float32), pltpu.VMEM((8, width), jnp.float32)],
        compiler_params=pltpu.CompilerParams(dimension_semantics=("arbitrary",), vmem_limit_bytes=VMEM),
        name=f"logits_{nt}",
    )(table, normed_t)


def grad_kernel(vocab, bv, rc, nt, own, info_ref, z_ref, e_ref, n_ref, lw_ref, w_ref, lab_ref, dt_ref, dn_ref, lz_ref, dz_ref, et_ref):
    i = pl.program_id(0)

    @pl.when(i == 0)
    def _():
        dn_ref[...] = jnp.zeros(dn_ref.shape, jnp.float32)
        lz_ref[...] = jnp.zeros(lz_ref.shape, jnp.float32)

    width = nt * TILE
    limit = vocab - i * bv
    labels = lab_ref[...] - i * bv
    lw = lw_ref[...]
    w = w_ref[...]
    for r in range(0, bv, rc):
        z = z_ref[pl.ds(r, rc), :]
        hit = lax.broadcasted_iota(jnp.int32, (rc, width), 0) + r == labels
        dz = (jnp.exp2(z - lw) - jnp.where(hit, w, 0.0)).astype(jnp.bfloat16)
        lz_ref[...] += jnp.sum(jnp.where(hit, z, 0.0).reshape(rc // 8, 8, width), axis=0)
        dz_ref[pl.ds(r, rc), :] = dz
        dt_ref[pl.ds(r, rc), :] = jnp.dot(dz, n_ref[...], preferred_element_type=jnp.float32)
        rows = lax.broadcasted_iota(jnp.int32, (rc, e_ref.shape[1]), 0) + r
        et_ref[:, pl.ds(r, rc)] = jnp.where(rows < limit, e_ref[pl.ds(r, rc), :], jnp.zeros((), jnp.bfloat16)).T
    for k in range(2, own + 1):
        @pl.when(info_ref[0] == k)
        def _():
            start = jnp.where(info_ref[1] == 0, 0, nt - k)
            cols = pl.ds(pl.multiple_of(start * TILE, TILE), k * TILE)
            dn_ref[:, :k * TILE] += jnp.dot(et_ref[...], dz_ref[:, cols], preferred_element_type=jnp.float32)


def grad_call(nt, bv, rc, own_max, info, z, table, normed, lw, w, labels):
    vocab, depth = table.shape
    steps = pl.cdiv(vocab, bv)
    width = nt * TILE
    full = normed.shape[0]
    own = min(nt, own_max)
    fixed = lambda i, *_: (0, 0)
    step = lambda i, *_: (i, 0)
    return pl.pallas_call(
        functools.partial(grad_kernel, vocab, bv, rc, nt, own),
        grid_spec=pltpu.PrefetchScalarGridSpec(
            num_scalar_prefetch=1,
            grid=(steps,),
            in_specs=[
                pl.BlockSpec((bv, width), step),
                pl.BlockSpec((bv, depth), step),
                pl.BlockSpec((width, depth), fixed),
                pl.BlockSpec((1, width), fixed),
                pl.BlockSpec((1, width), fixed),
                pl.BlockSpec((1, width), fixed),
            ],
            out_specs=[pl.BlockSpec((bv, depth), step), pl.BlockSpec((depth, own_max * TILE), fixed), pl.BlockSpec((8, width), fixed)],
            scratch_shapes=[pltpu.VMEM((bv, width), jnp.bfloat16), pltpu.VMEM((depth, bv), jnp.bfloat16)],
        ),
        out_shape=[
            jax.ShapeDtypeStruct((vocab, depth), jnp.float32),
            jax.ShapeDtypeStruct((depth, own_max * TILE), jnp.float32),
            jax.ShapeDtypeStruct((8, full), jnp.float32),
        ],
        compiler_params=pltpu.CompilerParams(dimension_semantics=("arbitrary",), vmem_limit_bytes=VMEM),
        name=f"grads_{nt}",
    )(info, z, table, normed, lw, w, labels)


MESH = pl.DeviceIdType.MESH


def greet(peers):
    barrier = pltpu.get_barrier_semaphore()
    for peer in peers:
        pl.semaphore_signal(barrier, inc=1, device_id=peer, device_id_type=MESH)
    pl.semaphore_wait(barrier, len(peers))


def remote(src, dst, sems, peer):
    return pltpu.make_async_remote_copy(
        src_ref=src, dst_ref=dst, send_sem=sems[0], recv_sem=sems[1], device_id=peer, device_id_type=MESH
    )


def neighbours():
    dp, vp = lax.axis_index("dp"), lax.axis_index("vp")
    core = vp + 1 - 2 * lax.rem(vp, 2)
    across = lax.rem(vp + 2, 4)
    other = {"dp": 1 - dp, "vp": vp}
    return dp, vp, across, other, {"dp": dp, "vp": core}, {"dp": dp, "vp": across}


def head_kernel(chunks, least, h_ref, gain_ref, marks_ref, n_ref, t_ref, row_ref, slot_ref, info_ref,
                land, pay, meta, their_meta, acc_n, acc_t, n_bf, send, recv, meta_send, meta_recv):
    dp, vp, across, other, core, cross = neighbours()
    own, depth = h_ref.shape
    total = 2 * own
    quarter = own // 4
    part = quarter // chunks
    barrier = pltpu.get_barrier_semaphore()
    for peer in (other, core, cross):
        pl.semaphore_signal(barrier, inc=1, device_id=peer, device_id_type=MESH)
    values = h_ref[...].astype(jnp.float32)
    centered = values - jnp.mean(values, axis=1, keepdims=True)
    var = jnp.mean(centered * centered, axis=1, keepdims=True)
    n_bf[...] = (gain_ref[...] * (centered * lax.rsqrt(var + EPS))).astype(jnp.bfloat16)
    pay[...] = n_bf[pl.ds(pl.multiple_of(vp * quarter, 16), quarter), :].astype(jnp.float32)
    flat = lambda at: jnp.concatenate([marks_ref[at + i:at + i + 1, :] for i in range(own // marks_ref.shape[1])], axis=1)
    mask = flat(0)
    code = jnp.where(mask > 0.0, flat(8), -1.0)
    upper = lax.broadcasted_iota(jnp.int32, (own, own), 0) <= lax.broadcasted_iota(jnp.int32, (own, own), 1)
    mask8 = jnp.broadcast_to(mask, (8, own)).astype(jnp.bfloat16)
    ranks = jnp.dot(mask8, upper.astype(jnp.float32).astype(jnp.bfloat16), preferred_element_type=jnp.float32)
    count = jnp.broadcast_to(jnp.sum(mask, axis=1, keepdims=True), (8, own))
    line = lax.broadcasted_iota(jnp.int32, (8, own), 0)
    meta[...] = jnp.where(line == 0, code, jnp.where(line == 1, ranks, count))
    pl.semaphore_wait(barrier, 3)
    swap = remote(meta, their_meta, (meta_send, meta_recv), other)
    swap.start()

    def copies(k):
        rows = pl.ds(pl.multiple_of(k * part, 8), part)
        sem = lambda hop: (send.at[hop, k], recv.at[hop, k])
        mine, theirs = land.at[vp, rows, :], land.at[across, rows, :]
        return (
            remote(pay.at[rows, :], mine, sem(0), other),
            remote(mine, mine, sem(1), core),
            remote(mine, mine, sem(2), cross),
            remote(theirs, theirs, sem(3), core),
        )

    for k in range(chunks):
        copies(k)[0].start()

    swap.wait_recv()
    c_own, c_other = meta[2:3, 0:1], their_meta[2:3, 0:1]
    ceil_tiles = lambda c: jnp.floor((c + (TILE - 1.0)) * (1.0 / TILE))
    tiles = jnp.maximum(ceil_tiles(c_own + c_other), float(least))
    widest = jnp.maximum(c_own, c_other)
    own_tiles = jnp.maximum(ceil_tiles(widest), 2.0)
    units = jnp.clip(jnp.floor((widest + 127.0) * (1.0 / 128.0)), 4.0, 6.0)
    lane = lax.broadcasted_iota(jnp.int32, info_ref.shape, 1)
    info = jnp.where(lane == 0, own_tiles, jnp.where(lane == 1, dp.astype(jnp.float32), jnp.where(lane == 2, tiles - float(least), units - 4.0)))
    info_ref[...] = info.astype(jnp.int32)

    def places(block, is_front):
        back = tiles * TILE - block[2:3, :]
        at = jnp.where(is_front, 0.0, back) + block[1:2, :] - 1.0
        at = jnp.where(block[0:1, :] >= 0.0, at, -1.0)
        both = jnp.where(line == 0, at, jnp.broadcast_to(block[0:1, :], (8, own)) + 1.0)
        return at, both.T

    my_row, my_cols = places(meta, dp == 0)
    my_col = my_cols[:, 0:1]
    base = jnp.where(dp == 0, 0.0, tiles * TILE - units * 128.0)
    slot_ref[...] = jnp.broadcast_to(jnp.where(my_col < 0.0, -1.0, my_col - base), slot_ref.shape)

    def pack(j, at_col, at_row, code_col, last):
        start = pl.multiple_of(j * TILE, TILE)
        offset = (j * TILE).astype(jnp.float32)
        lanes = lax.broadcasted_iota(jnp.int32, (own, TILE), 1).astype(jnp.float32) + offset
        subs = lax.broadcasted_iota(jnp.int32, (TILE, own), 0).astype(jnp.float32) + offset
        hot_t = at_col == lanes
        hot = (at_row == subs).astype(jnp.float32).astype(jnp.bfloat16)
        cut = pl.ds(start, TILE)
        labels = jnp.sum(jnp.where(hot_t, code_col, 0.0), axis=0, keepdims=True)
        hot_t = hot_t.astype(jnp.float32).astype(jnp.bfloat16)
        t = lax.dot_general(n_bf[...], hot_t, (((0,), (0,)), ((), ())), preferred_element_type=jnp.float32)
        n = jnp.dot(hot, n_bf[...], preferred_element_type=jnp.float32)
        if not last:
            acc_t[:, cut] = t
            acc_n[cut, :] = n
            row_ref[0:1, cut] = labels
        else:
            t_ref[:, cut] = (acc_t[:, cut] + t).astype(jnp.bfloat16)
            n_ref[cut, :] = (acc_n[cut, :] + n).astype(jnp.bfloat16)
            row_ref[0:1, cut] = row_ref[0:1, cut] + labels - 1.0

    @pl.loop(0, chunks)
    def _(k):
        first, to_core, to_cross, _ = copies(k)
        first.wait_recv()
        to_core.start()
        to_cross.start()

        @pl.when(k > 0)
        def _():
            _, _, arrived, relay = copies(k - 1)
            arrived.wait_recv()
            relay.start()

        pack(k, my_cols[:, 0:1], my_row, my_cols[:, 1:2], False)

    _, _, arrived, relay = copies(chunks - 1)
    arrived.wait_recv()
    relay.start()
    their_row, their_cols = places(their_meta, dp == 1)
    for k in range(chunks):
        _, to_core, _, relay = copies(k)
        to_core.wait_recv()
        relay.wait_recv()
    n_bf[...] = land[...].reshape(own, depth).astype(jnp.bfloat16)

    @pl.loop(0, total // TILE)
    def _(j):
        pack(j, their_cols[:, 0:1], their_row, their_cols[:, 1:2], True)

    swap.wait_send()
    for k in range(chunks):
        for copy in copies(k):
            copy.wait_send()


def head_call(h, gain, marks, least):
    own, depth = h.shape
    total = 2 * own
    chunks = total // TILE
    return pl.pallas_call(
        functools.partial(head_kernel, chunks, least),
        in_specs=[pl.BlockSpec(memory_space=pltpu.VMEM)] * 3,
        out_specs=[pl.BlockSpec(memory_space=pltpu.VMEM)] * 5,
        out_shape=[
            jax.ShapeDtypeStruct((total, depth), jnp.bfloat16),
            jax.ShapeDtypeStruct((depth, total), jnp.bfloat16),
            jax.ShapeDtypeStruct((8, total), jnp.float32),
            jax.ShapeDtypeStruct((own, 128), jnp.float32),
            jax.ShapeDtypeStruct((8, 128), jnp.int32),
        ],
        scratch_shapes=[
            pltpu.VMEM((4, own // 4, depth), jnp.float32),
            pltpu.VMEM((own // 4, depth), jnp.float32),
            pltpu.VMEM((8, own), jnp.float32),
            pltpu.VMEM((8, own), jnp.float32),
            pltpu.VMEM((total, depth), jnp.float32),
            pltpu.VMEM((depth, total), jnp.float32),
            pltpu.VMEM((own, depth), jnp.bfloat16),
            pltpu.SemaphoreType.DMA((4, chunks)),
            pltpu.SemaphoreType.DMA((4, chunks)),
            pltpu.SemaphoreType.DMA,
            pltpu.SemaphoreType.DMA,
        ],
        compiler_params=pltpu.CompilerParams(collective_id=0, has_side_effects=True, vmem_limit_bytes=VMEM),
        name="head",
    )(h, gain.reshape(1, depth), marks)


def stats_kernel(vocab, ms_ref, row_ref, lw_ref, w_ref, lab_ref, sum_ref, land, send, recv):
    dp, vp = lax.axis_index("dp"), lax.axis_index("vp")
    peers = [{"dp": dp, "vp": lax.rem(vp + k, 4)} for k in (1, 2, 3)]
    greet(peers)
    copies = [remote(ms_ref, land.at[vp], (send.at[k], recv.at[k]), peer) for k, peer in enumerate(peers)]
    for copy in copies:
        copy.start()
    land[vp] = ms_ref[...]
    labels = row_ref[0:1, :]
    live = labels >= 0.0
    count = jnp.sum(jnp.where(live, 1.0, 0.0), axis=1, keepdims=True)
    weight = LOGIT_SCALE / count
    rel = labels - (vp * vocab).astype(jnp.float32)
    lab_ref[...] = jnp.where(live & (rel < float(vocab)), rel, -1.0).astype(jnp.int32)
    w_ref[...] = jnp.where(live, weight, 0.0)
    for copy in copies:
        copy.wait()
    best = jnp.max(land[:, 0:1, :], axis=0)
    total = sum(land[k, 1:2, :] * jnp.exp2(land[k, 0:1, :] - best) for k in range(4))
    lse = best + jnp.log(total) * LOG2E
    lw_ref[...] = jnp.where(live, lse - jnp.log(weight) * LOG2E, -NEG)
    lse_sum = jnp.sum(jnp.where(live, lse, 0.0), axis=1, keepdims=True)
    sum_ref[...] = jnp.where(lax.broadcasted_iota(jnp.int32, sum_ref.shape, 1) == 0, lse_sum, count)


def stats_call(ms, row, vocab):
    total = ms.shape[1]
    line = lambda t: jax.ShapeDtypeStruct((1, total), t)
    return pl.pallas_call(
        functools.partial(stats_kernel, vocab),
        in_specs=[pl.BlockSpec(memory_space=pltpu.VMEM)] * 2,
        out_specs=[pl.BlockSpec(memory_space=pltpu.VMEM)] * 4,
        out_shape=[line(jnp.float32), line(jnp.float32), line(jnp.int32), jax.ShapeDtypeStruct((8, 128), jnp.float32)],
        scratch_shapes=[pltpu.VMEM((4, 8, total), jnp.float32), pltpu.SemaphoreType.DMA((3,)), pltpu.SemaphoreType.DMA((3,))],
        compiler_params=pltpu.CompilerParams(collective_id=1, has_side_effects=True),
        name="stats",
    )(ms, row)


def tail_kernel(chunks, slots, dn_ref, lz_ref, h_ref, gain_ref, slot_ref, w_ref, sum_ref, dh_ref, dg_ref, loss_ref,
                land1, part, land2, full, xhat, inv_ref, dh_t, pick, lz_land, gain_acc, gain_out, gain_in, send, recv, small_send, small_recv):
    dp, vp, across, other, core, cross = neighbours()
    c = lax.rem(vp, 2)
    halves, hrows, held = dn_ref.shape
    used = slots if slots % TILE == 0 else slots + 128
    window = pl.ds(pl.multiple_of(dp * (used - slots), 128), slots)
    depth = halves * hrows
    rows_k = hrows // chunks
    peers = [{"dp": dp, "vp": lax.rem(vp + k, 4)} for k in (1, 2, 3)]
    greet(peers + [other])
    lz_copies = [remote(lz_ref, lz_land.at[vp], (small_send.at[k], small_recv.at[k]), peer) for k, peer in enumerate(peers)]

    def copies(k):
        rows = pl.ds(pl.multiple_of(k * rows_k, 8), rows_k)
        sem = lambda hop: (send.at[hop, k], recv.at[hop, k])
        return rows, (
            remote(dn_ref.at[1 - c, rows, window], land1.at[rows, :], sem(0), core),
            remote(part.at[rows, :], land2.at[rows, :], sem(1), cross),
            remote(full.at[c, rows, :], full.at[c, rows, :], sem(2), core),
        )

    for k in range(chunks):
        copies(k)[1][0].start()

    @pl.loop(0, chunks)
    def _(k):
        rows, (swap, over, _) = copies(k)
        swap.wait_recv()
        part[rows, :] = dn_ref[c, rows, window] + land1[rows, :]
        over.start()

    for copy in lz_copies:
        copy.start()
    lz_land[vp] = lz_ref[...]
    tokens = h_ref.shape[0]

    def piece(j):
        return pl.ds(pl.multiple_of(j * 128, 128), 128)

    @pl.loop(0, slots // 128)
    def _(j):
        lanes = lax.broadcasted_iota(jnp.int32, (tokens, 128), 1).astype(jnp.float32) + (j * 128).astype(jnp.float32)
        hot = (lanes == slot_ref[...]).astype(jnp.float32).astype(jnp.bfloat16)
        pick[:, piece(j)] = hot
        h = lax.dot_general(h_ref[...], hot, (((0,), (0,)), ((), ())), preferred_element_type=jnp.float32)
        centered = h - jnp.mean(h, axis=0, keepdims=True)
        inv = lax.rsqrt(jnp.mean(centered * centered, axis=0, keepdims=True) + EPS)
        xhat[:, piece(j)] = centered * inv
        inv_ref[0:1, piece(j)] = inv

    @pl.loop(0, chunks)
    def _(k):
        rows, (_, over, back) = copies(k)
        over.wait_recv()
        full[c, rows, :] = part[rows, :] + land2[rows, :]
        back.start()

    for copy in lz_copies:
        copy.wait()
    for k in range(chunks):
        copies(k)[1][2].wait_recv()
    gain_col = jnp.broadcast_to(gain_ref[...], (8, depth)).T[:, 0:1]
    gain_acc[...] = jnp.zeros(gain_acc.shape, jnp.float32)

    @pl.loop(0, slots // 128)
    def _(j):
        dn = full[:, :, piece(j)].reshape(depth, 128)
        xh = xhat[:, piece(j)]
        gain_acc[...] += dn * xh
        a = dn * gain_col
        one = jnp.mean(a, axis=0, keepdims=True)
        two = jnp.mean(a * xh, axis=0, keepdims=True)
        dh_t[:, piece(j)] = (inv_ref[0:1, piece(j)] * (a - one - xh * two)).astype(jnp.bfloat16)

    gain_out[...] = jnp.broadcast_to(jnp.sum(gain_acc[...].T, axis=0, keepdims=True), gain_out.shape)
    share = remote(gain_out, gain_in, (small_send.at[3], small_recv.at[3]), other)
    share.start()

    @pl.loop(0, tokens // TILE)
    def _(j):
        rows = pl.ds(pl.multiple_of(j * TILE, TILE), TILE)
        dh = lax.dot_general(pick[rows, :], dh_t[...], (((1,), (1,)), ((), ())), preferred_element_type=jnp.float32)
        dh_ref[rows, :] = dh.astype(jnp.bfloat16)

    live = w_ref[...] > 0.0
    label_sum = jnp.zeros((1, 1), jnp.float32)
    for k in range(4):
        line = jnp.sum(lz_land[k], axis=0, keepdims=True)
        label_sum = label_sum + jnp.sum(jnp.where(live, line, 0.0), axis=1, keepdims=True)
    loss = (sum_ref[0:1, 0:1] - label_sum) * LN2 / sum_ref[0:1, 1:2]
    loss_ref[...] = jnp.broadcast_to(loss, loss_ref.shape)
    share.wait()
    dg_ref[...] = gain_out[...] + gain_in[...]
    for k in range(chunks):
        for copy in copies(k)[1]:
            copy.wait_send()


def tail_call(slots, cid, dn, lz, h, gain, slot, w, sums, chunks=7):
    tokens, depth = h.shape
    held = dn.shape[1]
    half = depth // 2
    return pl.pallas_call(
        functools.partial(tail_kernel, chunks, slots),
        in_specs=[pl.BlockSpec(memory_space=pltpu.VMEM)] * 7,
        out_specs=[pl.BlockSpec(memory_space=pltpu.VMEM)] * 3,
        out_shape=[
            jax.ShapeDtypeStruct((tokens, depth), jnp.bfloat16),
            jax.ShapeDtypeStruct((8, depth), jnp.float32),
            jax.ShapeDtypeStruct((8, 128), jnp.float32),
        ],
        scratch_shapes=[
            pltpu.VMEM((half, slots), jnp.float32),
            pltpu.VMEM((half, slots), jnp.float32),
            pltpu.VMEM((half, slots), jnp.float32),
            pltpu.VMEM((2, half, slots), jnp.float32),
            pltpu.VMEM((depth, slots), jnp.float32),
            pltpu.VMEM((8, slots), jnp.float32),
            pltpu.VMEM((depth, slots), jnp.bfloat16),
            pltpu.VMEM((tokens, slots), jnp.bfloat16),
            pltpu.VMEM((4, 8, lz.shape[1]), jnp.float32),
            pltpu.VMEM((depth, 128), jnp.float32),
            pltpu.VMEM((8, depth), jnp.float32),
            pltpu.VMEM((8, depth), jnp.float32),
            pltpu.SemaphoreType.DMA((3, chunks)),
            pltpu.SemaphoreType.DMA((3, chunks)),
            pltpu.SemaphoreType.DMA((4,)),
            pltpu.SemaphoreType.DMA((4,)),
        ],
        compiler_params=pltpu.CompilerParams(collective_id=cid, has_side_effects=True, vmem_limit_bytes=VMEM),
        name=f"tail_{slots}",
    )(dn.reshape(2, half, held), lz, h, gain.reshape(1, depth), slot, w, sums)


def solution(mesh):
    def local_step(hidden, norm_gain, emb_table, labels, tok_mask):
        rows, seq_len, depth = hidden.shape
        vocab_local = emb_table.shape[0]
        own = rows * seq_len
        flat = hidden.reshape(own, depth)
        pad = ((0, 8 - rows), (0, 0))
        marks = jnp.concatenate([jnp.pad(tok_mask, pad), jnp.pad(labels.astype(jnp.float32), pad)], axis=0)
        most = 2 * own // TILE
        variants = {nt: (1536 if nt < most else 256) for nt in range(2 * most // 3, most + 1)}
        z_rows = max(bv * pl.cdiv(vocab_local, bv) for bv in variants.values())
        packed, packed_t, line, slot, info = head_call(flat, norm_gain, marks, min(variants))
        which = jnp.clip(info[0, 2], 0, len(variants) - 1)
        z, ms = lax.switch(which, [functools.partial(logits_call, nt, bv, 128, z_rows) for nt, bv in variants.items()], emb_table, packed_t)
        lw, w, rel_labels, sums = stats_call(ms, line, vocab_local)
        d_table, dn_t, lz = lax.switch(
            which,
            [functools.partial(grad_call, nt, bv, 256, own // TILE) for nt, bv in variants.items()],
            info[0, :2], z, emb_table, packed, lw, w, rel_labels,
        )
        d_tokens, d_gain, loss = lax.switch(
            jnp.clip(info[0, 3], 0, 2),
            [functools.partial(tail_call, 512 + 128 * k, 2 + k) for k in range(3)],
            dn_t, lz, flat, norm_gain, slot, w, sums,
        )
        return loss[0, 0], d_table, d_tokens.reshape(rows, seq_len, depth), d_gain[0]

    return jax.shard_map(
        local_step,
        mesh=mesh,
        in_specs=(P("dp", None, None), P(None), P("vp", None), P("dp", None), P("dp", None)),
        out_specs=(P(), P("vp", None), P("dp", None, None), P(None)),
        check_vma=False,
    )
```
